64 devices in a mesh: dp: 8 (over x, y, core), tp: 8 (over z).
Axes of the slice: x: 2, y: 2, z: 8, core: 2. Of those that a mesh axis runs over, the one named last changes fastest.
The devices are a block of a 4x4x8 slice.
Arguments:
- x: bfloat16 [1024, 7168], P('dp'), parts along dimension 0
- w_gate: bfloat16 [7168, 20480], P(None, 'tp')
- w_up: bfloat16 [7168, 20480], P(None, 'tp')
- w_down: bfloat16 [20480, 7168], P('tp')
Outputs:
- output: bfloat16 [1024, 7168], P('dp'), parts along dimension 0
There are 8 independent parts. The reference program is written for one: setup_inputs(seed, part) draws one part's arguments, and reference() takes and returns one part's arrays. A program takes and returns all parts, laid end to end along the dimension named above; an argument that names none is the same for every part.
All inputs are finite; a program needn't handle non-finite values.
Results may differ from the reference program's by a relative error of at most 0.016.
Values are sent between devices in bfloat16 or wider.
A program may use at most 768 MiB of HBM per device.

```python
import jax
import jax.numpy as jnp

ROWS = 128
D = 7168
FF = 20480


def setup_inputs(seed: int = 0, part: int = 0) -> dict:
    kx, kg, ku, kd = jax.random.split(jax.random.key(seed), 4)
    drawn = {
        "x": jax.random.normal(jax.random.fold_in(kx, part), (ROWS, D), jnp.float32),
        "w_gate": jax.random.normal(kg, (D, FF), jnp.float32) * D**-0.5,
        "w_up": jax.random.normal(ku, (D, FF), jnp.float32) * D**-0.5,
        "w_down": jax.random.normal(kd, (FF, D), jnp.float32) * FF**-0.5,
    }
    return {k: v.astype(jnp.bfloat16) for k, v in drawn.items()}


def reference(x, w_gate, w_up, w_down):
    gate = jnp.dot(x, w_gate, preferred_element_type=jnp.float32)
    up = jnp.dot(x, w_up, preferred_element_type=jnp.float32)
    hidden = (jax.nn.silu(gate) * up).astype(jnp.bfloat16)
    return jnp.dot(hidden, w_down, preferred_element_type=jnp.float32).astype(jnp.bfloat16)
```

```python
import functools

import jax
import jax.numpy as jnp
from jax import lax
from jax.experimental import pallas as pl
from jax.experimental.pallas import tpu as pltpu
from jax.sharding import PartitionSpec as P

MESH = pl.DeviceIdType.MESH
F32, BF16 = jnp.float32, jnp.bfloat16

BLOCK = 256
HALVES = 2
SLOTS = 4
DOWN_SLOTS = 4
PIECES = 4

FIRST = ((0, 1), (2, 3))
SECOND = ((2, 3, 0, 1), (0, 1, 2, 3))
LATER = ((2, 0, 3, 1), (0, 2, 1, 3))
FINAL = (0, 2, 1, 3)
LAST = ((0, 1), (2, 3))


def reduce_plan(hops):
    plans = []
    for way in range(2):
        plan = [(1, r) for r in FIRST[way]] + [(2, r) for r in SECOND[way]]
        for hop in range(3, hops + 1):
            plan += [(hop, r) for r in LATER[way]]
        plans.append(plan)
    return plans


def gather_plan(hops):
    plans = []
    for way in range(2):
        plan = [(hop, r) for hop in range(1, hops) for r in FINAL]
        plans.append(plan + [(hops, r) for r in LAST[way]])
    return plans


def kernel(
    n, x_ref, wg_ref, wu_ref, wd_ref, y_ref,
    xs, gbuf, ubuf, acc_g, acc_u, hid, hout, dbuf, part, rs_out, rs_in,
    x_sem, xr_send, xr_recv, w_sem, h_send, h_recv, d_sem,
    rs_send, rs_recv, ag_send, ag_recv,
):
    rows, depth = x_ref.shape
    cols = wg_ref.shape[1]
    mine = cols // 2
    blocks = mine // BLOCK
    kd = depth // HALVES
    steps = blocks * HALVES
    chunk = depth // n
    hops = n // 2
    height = rows // PIECES

    tp = lax.axis_index("tp")
    dp = lax.axis_index("dp")
    core = lax.rem(dp, 2)
    partner = {"dp": dp + 1 - 2 * core}
    ways = ({"tp": lax.rem(tp + 1, n)}, {"tp": lax.rem(tp + n - 1, n)})
    my_cols = core * mine
    other_cols = mine - my_cols

    def x_copy(h):
        ks = pl.ds(h * kd, kd)
        return pltpu.make_async_copy(x_ref.at[:, ks], xs.at[pl.ds(0, rows), ks], x_sem.at[h])

    def x_remote(h):
        ks = pl.ds(h * kd, kd)
        return pltpu.make_async_remote_copy(
            src_ref=x_ref.at[:, ks], dst_ref=xs.at[pl.ds(rows, rows), ks],
            send_sem=xr_send.at[h], recv_sem=xr_recv.at[h], device_id=partner, device_id_type=MESH,
        )

    def w_copies(step):
        b, h, slot = step // HALVES, step % HALVES, step % SLOTS
        ks = pl.ds(pl.multiple_of(h * kd, kd), kd)
        ns = pl.ds(pl.multiple_of(my_cols + b * BLOCK, BLOCK), BLOCK)
        return (
            pltpu.make_async_copy(wg_ref.at[ks, ns], gbuf.at[slot], w_sem.at[0, slot]),
            pltpu.make_async_copy(wu_ref.at[ks, ns], ubuf.at[slot], w_sem.at[1, slot]),
        )

    def w_start(step):
        for c in w_copies(step):
            c.start()

    def w_wait(step):
        for c in w_copies(step):
            c.wait()

    def chunk_at(k):
        offset = hops if k == 0 else (n if k == n - 1 else (hops - (k + 1) // 2 if k % 2 else n - hops + k // 2))
        return lax.rem(tp + offset, n)

    def columns(c):
        return pl.ds(pl.multiple_of(c * chunk, chunk), chunk)

    def d_copies(k):
        cs = columns(chunk_at(k))
        slot = k % DOWN_SLOTS
        return [
            pltpu.make_async_copy(
                wd_ref.at[pl.ds(pl.multiple_of(o, mine), mine), cs],
                dbuf.at[slot, pl.ds(i * mine, mine)], d_sem.at[slot, i],
            )
            for i, o in enumerate((my_cols, other_cols))
        ]

    def h_copy(b):
        where = pl.ds(pl.multiple_of(mine + b * BLOCK, BLOCK), BLOCK)
        return pltpu.make_async_remote_copy(
            src_ref=hout.at[b], dst_ref=hid.at[:, where],
            send_sem=h_send.at[b], recv_sem=h_recv.at[b], device_id=partner, device_id_type=MESH,
        )

    x_copy(0).start()
    w_start(0)
    x_copy(1).start()
    for s in range(1, SLOTS):
        w_start(s)

    barrier = pltpu.get_barrier_semaphore()
    for who in (partner,) + ways:
        pl.semaphore_signal(barrier, inc=1, device_id=who, device_id_type=MESH)
    pl.semaphore_wait(barrier, 3)
    for h in range(HALVES):
        x_remote(h).start()

    def dot(a, b):
        return jnp.dot(a, b, preferred_element_type=F32)

    def finish(b, gate, up, half):
        hidden = (jax.nn.silu(gate) * up).astype(BF16)
        if half != 1:
            hid[:, pl.ds(pl.multiple_of(b * BLOCK, BLOCK), BLOCK)] = hidden[:rows]
        if half != 0:
            hout[b] = hidden[-rows:]
            h_copy(b).start()

    def half_step(b, h, half):
        rs = pl.ds(half * rows, rows)
        lhs = xs[rs, pl.ds(h * kd, kd)]
        gate, up = dot(lhs, gbuf[h]), dot(lhs, ubuf[h])
        if h == 0:
            acc_g[rs] = gate
            acc_u[rs] = up
        else:
            finish(b, acc_g[rs] + gate, acc_u[rs] + up, half)

    for half in range(2):
        for h in range(HALVES):
            if half == 0:
                x_copy(h).wait()
                w_wait(h)
            else:
                x_remote(h).wait_recv()
            half_step(0, h, half)
            if half == 1:
                w_start(h + SLOTS)

    @pl.loop(1, blocks)
    def _(b):
        for h in range(HALVES):
            step = b * HALVES + h
            slot = lax.rem(step, SLOTS)
            w_wait(step)
            lhs = xs[:, pl.ds(h * kd, kd)]
            gate, up = dot(lhs, gbuf[slot]), dot(lhs, ubuf[slot])
            if h == 0:
                acc_g[...] = gate
                acc_u[...] = up
            else:
                finish(b, acc_g[...] + gate, acc_u[...] + up, 2)

            @pl.when(step + SLOTS < steps)
            def _():
                w_start(step + SLOTS)

            for k in range(DOWN_SLOTS):
                @pl.when(step + SLOTS == steps + k)
                def _():
                    for c in d_copies(k):
                        c.start()

    def compute(k):
        slot = k % DOWN_SLOTS
        for i, c in enumerate(d_copies(k)):
            c.wait()
            if k == 0:
                ks = pl.ds(i * mine, mine)
                if i == 1:
                    for b in range(blocks):
                        h_copy(b).wait_recv()
                p = dot(hid[:, ks], dbuf[slot, ks])
                part[k] = p if i == 0 else part[k] + p
        if k > 0:
            part[k] = dot(hid[...], dbuf[slot])
        if k + DOWN_SLOTS < n:
            for c in d_copies(k + DOWN_SLOTS):
                c.start()

    plan = reduce_plan(hops)
    place = [{m: q for q, m in enumerate(p)} for p in plan]

    def rs_copy(way, q):
        return pltpu.make_async_remote_copy(
            src_ref=rs_out.at[way, q], dst_ref=rs_in.at[way, q],
            send_sem=rs_send.at[way, q], recv_sem=rs_recv.at[way, q],
            device_id=ways[way], device_id_type=MESH,
        )

    def place_of(way, hop):
        return 0 if hop == 1 else 2 * (hop - 1) - 1 + way

    def reduce_send(way, hop, r):
        q = place[way][hop, r]
        term = part[place_of(way, hop), pl.ds(r * height, height)]
        before = place[way].get((hop - 1, r))
        if before is not None:
            rs_copy(way, before).wait_recv()
            term = term + rs_in[way, before].astype(F32)
        rs_out[way, q] = term.astype(BF16)
        rs_copy(way, q).start()

    def reduce_hop(hop, picked):
        for i in picked:
            for way in range(2):
                order = [r for (h, r) in plan[way] if h == hop]
                reduce_send(way, hop, order[i])

    compute(0)
    reduce_hop(1, range(PIECES // 2))
    compute(1)
    for r in SECOND[0][: PIECES // 2]:
        reduce_send(0, 2, r)
    compute(2)
    for r in SECOND[1][: PIECES // 2]:
        reduce_send(1, 2, r)
    for k in range(3, min(5, n)):
        compute(k)
    reduce_hop(2, range(PIECES // 2, PIECES))
    for k in range(5, n - 1):
        compute(k)
    if hops > 2:
        reduce_hop(3, range(PIECES))
    compute(n - 1)
    for hop in range(4, hops + 1):
        reduce_hop(hop, range(PIECES))

    gplan = gather_plan(hops)
    gplace = [{m: q for q, m in enumerate(p)} for p in gplan]

    def ag_copy(way, hop, r):
        q = gplace[way][hop, r]
        back = hop - 1
        owner = lax.rem(tp + (n - back if way == 0 else back), n)
        where = y_ref.at[pl.ds(r * height, height), columns(owner)]
        return pltpu.make_async_remote_copy(
            src_ref=where, dst_ref=where, send_sem=ag_send.at[way, q], recv_sem=ag_recv.at[way, q],
            device_id=ways[way], device_id_type=MESH,
        )

    def ag_arrival(way, hop, r):
        q = gplace[way][hop, r]
        owner = lax.rem(tp + (n - hop if way == 0 else hop), n)
        where = y_ref.at[pl.ds(r * height, height), columns(owner)]
        return pltpu.make_async_remote_copy(
            src_ref=where, dst_ref=where, send_sem=ag_send.at[way, q], recv_sem=ag_recv.at[way, q],
            device_id=ways[way], device_id_type=MESH,
        )

    own = columns(tp)
    for r in FINAL:
        rs = pl.ds(r * height, height)
        total = part[n - 1, rs]
        for way in range(2):
            q = place[way][hops, r]
            rs_copy(way, q).wait_recv()
            total = total + rs_in[way, q].astype(F32)
        y_ref[rs, own] = total.astype(BF16)
        for way in range(2):
            ag_copy(way, 1, r).start()
    for hop in range(1, hops + 1):
        for r in FINAL:
            for way in range(2):
                if (hop, r) in gplace[way]:
                    ag_arrival(way, hop, r).wait_recv()
                    if (hop + 1, r) in gplace[way]:
                        ag_copy(way, hop + 1, r).start()

    for h in range(HALVES):
        x_remote(h).wait_send()
    for b in range(blocks):
        h_copy(b).wait_send()
    for way in range(2):
        for q in range(len(plan[way])):
            rs_copy(way, q).wait_send()
        for hop, r in gplan[way]:
            ag_copy(way, hop, r).wait_send()


def solution(mesh):
    n = mesh.shape["tp"]

    def step(x, w_gate, w_up, w_down):
        rows, depth = x.shape
        cols = w_gate.shape[1]
        mine = cols // 2
        blocks = mine // BLOCK
        kd = depth // HALVES
        chunk = depth // n
        height = rows // PIECES
        messages = len(reduce_plan(n // 2)[0])
        hbm = pl.BlockSpec(memory_space=pltpu.HBM)
        dma = pltpu.SemaphoreType.DMA
        return pl.pallas_call(
            functools.partial(kernel, n),
            out_shape=jax.ShapeDtypeStruct((rows, depth), BF16),
            in_specs=[hbm] * 4,
            out_specs=pl.BlockSpec(memory_space=pltpu.VMEM),
            scratch_shapes=[
                pltpu.VMEM((2 * rows, depth), BF16),
                pltpu.VMEM((SLOTS, kd, BLOCK), BF16),
                pltpu.VMEM((SLOTS, kd, BLOCK), BF16),
                pltpu.VMEM((2 * rows, BLOCK), F32),
                pltpu.VMEM((2 * rows, BLOCK), F32),
                pltpu.VMEM((rows, cols), BF16),
                pltpu.VMEM((blocks, rows, BLOCK), BF16),
                pltpu.VMEM((DOWN_SLOTS, cols, chunk), BF16),
                pltpu.VMEM((n, rows, chunk), F32),
                pltpu.VMEM((2, messages, height, chunk), BF16),
                pltpu.VMEM((2, messages, height, chunk), BF16),
                dma((HALVES,)), dma((HALVES,)), dma((HALVES,)),
                dma((2, SLOTS)), dma((blocks,)), dma((blocks,)),
                dma((DOWN_SLOTS, 2)),
                dma((2, messages)), dma((2, messages)), dma((2, messages)), dma((2, messages)),
            ],
            compiler_params=pltpu.CompilerParams(
                collective_id=0, has_side_effects=True, vmem_limit_bytes=64 * 1024 * 1024 - 65536,
            ),
        )(x, w_gate, w_up, w_down)

    return jax.shard_map(
        step,
        mesh=mesh,
        in_specs=(P("dp", None), P(None, "tp"), P(None, "tp"), P("tp", None)),
        out_specs=P("dp", None),
        check_vma=False,
    )
```

```python
import functools

import jax
import jax.numpy as jnp
from jax import lax
from jax.experimental import pallas as pl
from jax.experimental.pallas import tpu as pltpu
from jax.sharding import PartitionSpec as P

MESH = pl.DeviceIdType.MESH
F32, BF16 = jnp.float32, jnp.bfloat16

TILE = 256
PARTS = 4
SLOTS = 12
AHEAD = 3
DOWN_SLOTS = 4
PIECES = 4

LOWER, UPPER = tuple(range(PIECES // 2)), tuple(range(PIECES // 2, PIECES))


def mixed(a, b):
    return tuple(r for pair in zip(a, b) for r in pair)


FIRST = (LOWER, UPPER)
SECOND = (UPPER + LOWER, LOWER + UPPER)
LATER = (mixed(UPPER, LOWER), mixed(LOWER, UPPER))
FINAL = mixed(LOWER, UPPER)
LAST = (LOWER, UPPER)


def reduce_plan(hops):
    plans = []
    for way in range(2):
        plan = [(1, r) for r in FIRST[way]] + [(2, r) for r in SECOND[way]]
        for hop in range(3, hops + 1):
            plan += [(hop, r) for r in LATER[way]]
        plans.append(plan)
    return plans


def gather_plan(hops):
    plans = []
    for way in range(2):
        plan = [(hop, r) for hop in range(1, hops) for r in FINAL]
        plans.append(plan + [(hops, r) for r in LAST[way]])
    return plans


def kernel(
    n, x_ref, wg_ref, wu_ref, wd_ref, y_ref,
    xs, gbuf, ubuf, gacc, uacc, hid, hout, dbuf, part, rs_out, rs_in,
    x_sem, xr_send, xr_recv, w_sem, h_send, h_recv, d_sem,
    rs_send, rs_recv, ag_send, ag_recv,
):
    rows, depth = x_ref.shape
    cols = wg_ref.shape[1]
    mine = cols // 2
    blocks = mine // TILE
    kd = depth // PARTS
    tiles = kd // TILE
    steps = blocks * PARTS
    chunk = depth // n
    hops = n // 2
    height = rows // PIECES

    tp = lax.axis_index("tp")
    dp = lax.axis_index("dp")
    core = lax.rem(dp, 2)
    partner = {"dp": dp + 1 - 2 * core}
    ways = ({"tp": lax.rem(tp + 1, n)}, {"tp": lax.rem(tp + n - 1, n)})
    my_cols = core * mine
    other_cols = mine - my_cols

    def x_copy(h):
        ks = pl.ds(h * kd, kd)
        return pltpu.make_async_copy(x_ref.at[:, ks], xs.at[pl.ds(0, rows), ks], x_sem.at[h])

    def x_remote(h):
        ks = pl.ds(h * kd, kd)
        return pltpu.make_async_remote_copy(
            src_ref=xs.at[pl.ds(0, rows), ks], dst_ref=xs.at[pl.ds(rows, rows), ks],
            send_sem=xr_send.at[h], recv_sem=xr_recv.at[h], device_id=partner, device_id_type=MESH,
        )

    def w_copies(step):
        b, h, slot = step // PARTS, step % PARTS, step % SLOTS
        ks = pl.ds(h * kd, kd)
        ns = pl.ds(pl.multiple_of(my_cols + b * TILE, TILE), TILE)
        return (
            pltpu.make_async_copy(wg_ref.at[ks, ns], gbuf.at[slot], w_sem.at[0, slot]),
            pltpu.make_async_copy(wu_ref.at[ks, ns], ubuf.at[slot], w_sem.at[1, slot]),
        )

    def chunk_at(k):
        offset = hops if k == 0 else (n if k == n - 1 else (hops - (k + 1) // 2 if k % 2 else n - hops + k // 2))
        return lax.rem(tp + offset, n)

    def columns(c):
        return pl.ds(pl.multiple_of(c * chunk, chunk), chunk)

    def d_copy(k, i):
        slot = k % DOWN_SLOTS
        o = (my_cols, other_cols)[i]
        return pltpu.make_async_copy(
            wd_ref.at[pl.ds(pl.multiple_of(o, mine), mine), columns(chunk_at(k))],
            dbuf.at[slot, pl.ds(i * mine, mine)], d_sem.at[slot, i],
        )

    def h_copy(b):
        return pltpu.make_async_remote_copy(
            src_ref=hout.at[b], dst_ref=hid.at[:, pl.ds(mine + b * TILE, TILE)],
            send_sem=h_send.at[b], recv_sem=h_recv.at[b], device_id=partner, device_id_type=MESH,
        )

    loads = [w_copies(s) for s in range(steps)] + [
        (d_copy(k, i),) for k in range(DOWN_SLOTS) for i in range(2)
    ]

    def start_load(j):
        if j < len(loads):
            for c in loads[j]:
                c.start()

    for h in range(PARTS):
        x_copy(h).start()
    for j in range(AHEAD):
        start_load(j)

    barrier = pltpu.get_barrier_semaphore()
    for who in (partner,) + ways:
        pl.semaphore_signal(barrier, inc=1, device_id=who, device_id_type=MESH)

    pl.semaphore_wait(barrier, 3)
    for h in range(PARTS):
        x_copy(h).wait()
        x_remote(h).start()

    def dot(a, b):
        return jnp.dot(a, b, preferred_element_type=F32)

    def arrive(b, h):
        for c in w_copies(b * PARTS + h):
            c.wait()

    def multiply(b, first, count, at, size):
        rs = pl.ds(at, size)
        lhs = xs[rs, pl.ds(first * kd, count * kd)]
        slot = (b * PARTS + first) % SLOTS
        for buf, acc in ((gbuf, gacc), (ubuf, uacc)):
            product = dot(lhs, buf[pl.ds(slot, count)].reshape(count * kd, TILE))
            acc[b % 2, rs] = product if first == 0 else acc[b % 2, rs] + product

    def hidden(b, half):
        rs = pl.ds(half * rows, rows)
        value = (jax.nn.silu(gacc[b % 2, rs]) * uacc[b % 2, rs]).astype(BF16)
        if half == 0:
            hid[:, pl.ds(b * TILE, TILE)] = value
        else:
            hout[b] = value

    for h in range(PARTS):
        arrive(0, h)
        for j in range(AHEAD + 2 * h, SLOTS if h == PARTS - 1 else min(AHEAD + 2 * h + 2, SLOTS)):
            start_load(j)
        multiply(0, h, 1, 0, rows)
    for h in range(0, PARTS, 2):
        for i in range(2):
            x_remote(h + i).wait_recv()
        multiply(0, h, 2, rows, rows)
        for i in range(2):
            start_load(h + i + SLOTS)
    for b in range(1, blocks):
        for part_of, count in ((0, PARTS // 2), (PARTS // 2, PARTS // 2)) if b == blocks - 1 else ((0, PARTS),):
            for h in range(part_of, part_of + count):
                arrive(b, h)
            multiply(b, part_of, count, 0, 2 * rows)
            if part_of == 0:
                hidden(b - 1, 1)
                hidden(b - 1, 0)
            for h in range(part_of, part_of + count):
                start_load(b * PARTS + h + SLOTS)
            if part_of == 0:
                h_copy(b - 1).start()
    hidden(blocks - 1, 1)
    h_copy(blocks - 1).start()
    hidden(blocks - 1, 0)

    def compute(k):
        slot = k % DOWN_SLOTS
        if k == 0:
            early = cols - TILE
            d_copy(k, 0).wait()
            d_copy(k, 1).wait()
            for b in range(blocks - 1):
                h_copy(b).wait_recv()
            part[k] = dot(hid[:, pl.ds(0, early)], dbuf[slot, pl.ds(0, early)])
            h_copy(blocks - 1).wait_recv()
            part[k] = part[k] + dot(hid[:, pl.ds(early, TILE)], dbuf[slot, pl.ds(early, TILE)])
        else:
            for i in range(2):
                d_copy(k, i).wait()
            part[k] = dot(hid[...], dbuf[slot])
        if k + DOWN_SLOTS < n:
            for i in range(2):
                d_copy(k + DOWN_SLOTS, i).start()

    plan = reduce_plan(hops)
    place = [{m: q for q, m in enumerate(p)} for p in plan]

    def rs_copy(way, q):
        return pltpu.make_async_remote_copy(
            src_ref=rs_out.at[way, q], dst_ref=rs_in.at[way, q],
            send_sem=rs_send.at[way, q], recv_sem=rs_recv.at[way, q],
            device_id=ways[way], device_id_type=MESH,
        )

    def place_of(way, hop):
        return 0 if hop == 1 else 2 * (hop - 1) - 1 + way

    def reduce_send(way, hop, r):
        q = place[way][hop, r]
        term = part[place_of(way, hop), pl.ds(r * height, height)]
        before = place[way].get((hop - 1, r))
        if before is not None:
            rs_copy(way, before).wait_recv()
            term = term + rs_in[way, before].astype(F32)
        rs_out[way, q] = term.astype(BF16)
        rs_copy(way, q).start()

    def reduce_hop(hop, picked):
        for i in picked:
            for way in range(2):
                order = [r for (h, r) in plan[way] if h == hop]
                reduce_send(way, hop, order[i])

    compute(0)
    reduce_hop(1, range(PIECES // 2))
    compute(1)
    for r in SECOND[0][: PIECES // 2]:
        reduce_send(0, 2, r)
    compute(2)
    for r in SECOND[1][: PIECES // 2]:
        reduce_send(1, 2, r)
    for k in range(3, min(5, n)):
        compute(k)
    reduce_hop(2, range(PIECES // 2, PIECES))
    for k in range(5, n - 1):
        compute(k)
    if hops > 2:
        reduce_hop(3, range(PIECES))
    compute(n - 1)
    for hop in range(4, hops + 1):
        reduce_hop(hop, range(PIECES))

    gplan = gather_plan(hops)
    gplace = [{m: q for q, m in enumerate(p)} for p in gplan]

    def ag_copy(way, hop, r):
        q = gplace[way][hop, r]
        back = hop - 1
        owner = lax.rem(tp + (n - back if way == 0 else back), n)
        where = y_ref.at[pl.ds(r * height, height), columns(owner)]
        return pltpu.make_async_remote_copy(
            src_ref=where, dst_ref=where, send_sem=ag_send.at[way, q], recv_sem=ag_recv.at[way, q],
            device_id=ways[way], device_id_type=MESH,
        )

    def ag_arrival(way, hop, r):
        q = gplace[way][hop, r]
        owner = lax.rem(tp + (n - hop if way == 0 else hop), n)
        where = y_ref.at[pl.ds(r * height, height), columns(owner)]
        return pltpu.make_async_remote_copy(
            src_ref=where, dst_ref=where, send_sem=ag_send.at[way, q], recv_sem=ag_recv.at[way, q],
            device_id=ways[way], device_id_type=MESH,
        )

    own = columns(tp)
    for r in FINAL:
        rs = pl.ds(r * height, height)
        total = part[n - 1, rs]
        for way in range(2):
            q = place[way][hops, r]
            rs_copy(way, q).wait_recv()
            total = total + rs_in[way, q].astype(F32)
        y_ref[rs, own] = total.astype(BF16)
        for way in range(2):
            ag_copy(way, 1, r).start()
    for hop in range(1, hops + 1):
        for r in FINAL:
            for way in range(2):
                if (hop, r) in gplace[way]:
                    ag_arrival(way, hop, r).wait_recv()
                    if (hop + 1, r) in gplace[way]:
                        ag_copy(way, hop + 1, r).start()

    for h in range(PARTS):
        x_remote(h).wait_send()
    for b in range(blocks):
        h_copy(b).wait_send()
    for way in range(2):
        for q in range(len(plan[way])):
            rs_copy(way, q).wait_send()
        for hop, r in gplan[way]:
            ag_copy(way, hop, r).wait_send()


def solution(mesh):
    n = mesh.shape["tp"]

    def step(x, w_gate, w_up, w_down):
        rows, depth = x.shape
        cols = w_gate.shape[1]
        mine = cols // 2
        blocks = mine // TILE
        kd = depth // PARTS
        chunk = depth // n
        height = rows // PIECES
        messages = len(reduce_plan(n // 2)[0])
        hbm = pl.BlockSpec(memory_space=pltpu.HBM)
        dma = pltpu.SemaphoreType.DMA
        return pl.pallas_call(
            functools.partial(kernel, n),
            out_shape=pltpu.VMEM((rows, depth), BF16),
            in_specs=[hbm] * 4,
            out_specs=pl.BlockSpec(memory_space=pltpu.VMEM),
            scratch_shapes=[
                pltpu.VMEM((2 * rows, depth), BF16),
                pltpu.VMEM((SLOTS, kd, TILE), BF16),
                pltpu.VMEM((SLOTS, kd, TILE), BF16),
                pltpu.VMEM((2, 2 * rows, TILE), F32),
                pltpu.VMEM((2, 2 * rows, TILE), F32),
                pltpu.VMEM((rows, cols), BF16),
                pltpu.VMEM((blocks, rows, TILE), BF16),
                pltpu.VMEM((DOWN_SLOTS, cols, chunk), BF16),
                pltpu.VMEM((n, rows, chunk), F32),
                pltpu.VMEM((2, messages, height, chunk), BF16),
                pltpu.VMEM((2, messages, height, chunk), BF16),
                dma((PARTS,)), dma((PARTS,)), dma((PARTS,)),
                dma((2, SLOTS)), dma((blocks,)), dma((blocks,)),
                dma((DOWN_SLOTS, 2)),
                dma((2, messages)), dma((2, messages)), dma((2, messages)), dma((2, messages)),
            ],
            compiler_params=pltpu.CompilerParams(
                collective_id=0, has_side_effects=True, vmem_limit_bytes=56 * 1024 * 1024,
            ),
        )(x, w_gate, w_up, w_down)

    return jax.shard_map(
        step,
        mesh=mesh,
        in_specs=(P("dp", None), P(None, "tp"), P(None, "tp"), P("tp", None)),
        out_specs=P("dp", None),
        check_vma=False,
    )
```

```python
import functools

import jax
import jax.numpy as jnp
from jax import lax
from jax.experimental import pallas as pl
from jax.experimental.pallas import tpu as pltpu
from jax.sharding import PartitionSpec as P

MESH = pl.DeviceIdType.MESH
F32, BF16 = jnp.float32, jnp.bfloat16

TILE = 256
PARTS = 4
SLOTS = 12
START = 3
AHEAD = 5
EARLY = 1
DOWN_SLOTS = 4
PIECES = 4

LOWER, UPPER = tuple(range(PIECES // 2)), tuple(range(PIECES // 2, PIECES))


def mixed(a, b):
    return tuple(r for pair in zip(a, b) for r in pair)


FIRST = (LOWER, UPPER)
SECOND = (UPPER + LOWER, LOWER + UPPER)
LATER = (mixed(UPPER, LOWER), mixed(LOWER, UPPER))
FINAL = mixed(LOWER, UPPER)
LAST = (LOWER, UPPER)


def reduce_plan(hops):
    plans = []
    for way in range(2):
        plan = [(1, r) for r in FIRST[way]] + [(2, r) for r in SECOND[way]]
        for hop in range(3, hops + 1):
            plan += [(hop, r) for r in LATER[way]]
        plans.append(plan)
    return plans


def gather_plan(hops):
    plans = []
    for way in range(2):
        plan = [(hop, r) for hop in range(1, hops) for r in FINAL]
        plans.append(plan + [(hops, r) for r in LAST[way]])
    return plans


def kernel(
    n, x_ref, wg_ref, wu_ref, wd_ref, y_ref,
    xs, gbuf, ubuf, gacc, uacc, hid, hout, dbuf, part, rs_out, rs_in,
    x_sem, xr_send, xr_recv, w_sem, h_send, h_recv, d_sem,
    rs_send, rs_recv, ag_send, ag_recv,
):
    rows, depth = x_ref.shape
    cols = wg_ref.shape[1]
    mine = cols // 2
    blocks = mine // TILE
    kd = depth // PARTS
    tiles = kd // TILE
    steps = blocks * PARTS
    chunk = depth // n
    hops = n // 2
    height = rows // PIECES

    tp = lax.axis_index("tp")
    dp = lax.axis_index("dp")
    core = lax.rem(dp, 2)
    partner = {"dp": dp + 1 - 2 * core}
    ways = ({"tp": lax.rem(tp + 1, n)}, {"tp": lax.rem(tp + n - 1, n)})
    my_cols = core * mine
    other_cols = mine - my_cols

    def x_copy(h):
        ks = pl.ds(h * kd, kd)
        return pltpu.make_async_copy(x_ref.at[:, ks], xs.at[pl.ds(0, rows), ks], x_sem.at[h])

    def x_remote(h):
        ks = pl.ds(h * kd, kd)
        return pltpu.make_async_remote_copy(
            src_ref=xs.at[pl.ds(0, rows), ks], dst_ref=xs.at[pl.ds(rows, rows), ks],
            send_sem=xr_send.at[h], recv_sem=xr_recv.at[h], device_id=partner, device_id_type=MESH,
        )

    def w_copies(step):
        b, h, slot = step // PARTS, step % PARTS, step % SLOTS
        ks = pl.ds(h * kd, kd)
        ns = pl.ds(pl.multiple_of(my_cols + b * TILE, TILE), TILE)
        return (
            pltpu.make_async_copy(wg_ref.at[ks, ns], gbuf.at[slot], w_sem.at[0, slot]),
            pltpu.make_async_copy(wu_ref.at[ks, ns], ubuf.at[slot], w_sem.at[1, slot]),
        )

    def chunk_at(k):
        offset = hops if k == 0 else (n if k == n - 1 else (hops - (k + 1) // 2 if k % 2 else n - hops + k // 2))
        return lax.rem(tp + offset, n)

    def columns(c):
        return pl.ds(pl.multiple_of(c * chunk, chunk), chunk)

    def d_copy(k, i):
        slot = k % DOWN_SLOTS
        o = (my_cols, other_cols)[i]
        return pltpu.make_async_copy(
            wd_ref.at[pl.ds(pl.multiple_of(o, mine), mine), columns(chunk_at(k))],
            dbuf.at[slot, pl.ds(i * mine, mine)], d_sem.at[slot, i],
        )

    def h_copy(b):
        return pltpu.make_async_remote_copy(
            src_ref=hout.at[b], dst_ref=hid.at[:, pl.ds(mine + b * TILE, TILE)],
            send_sem=h_send.at[b], recv_sem=h_recv.at[b], device_id=partner, device_id_type=MESH,
        )

    loads = [w_copies(s) for s in range(steps)] + [
        (d_copy(k, i),) for k in range(DOWN_SLOTS) for i in range(2)
    ]
    asked, freed = [0], [0]

    def ask(upto):
        while asked[0] < min(upto, len(loads)) and (asked[0] >= steps or asked[0] < freed[0] + SLOTS):
            for c in loads[asked[0]]:
                c.start()
            asked[0] += 1

    for h in range(PARTS):
        x_copy(h).start()
        ask(min(h + 1, START))

    barrier = pltpu.get_barrier_semaphore()
    for who in (partner,) + ways:
        pl.semaphore_signal(barrier, inc=1, device_id=who, device_id_type=MESH)

    pl.semaphore_wait(barrier, 3)

    def dot(a, b):
        return jnp.dot(a, b, preferred_element_type=F32)

    def arrive(b, h):
        for c in w_copies(b * PARTS + h):
            c.wait()

    def multiply(b, first, count, at, size):
        rs = pl.ds(at, size)
        lhs = xs[rs, pl.ds(first * kd, count * kd)]
        slot = (b * PARTS + first) % SLOTS
        for buf, acc in ((gbuf, gacc), (ubuf, uacc)):
            product = dot(lhs, buf[pl.ds(slot, count)].reshape(count * kd, TILE))
            acc[b % 2, rs] = product if first == 0 else acc[b % 2, rs] + product

    def hidden(b, half):
        rs = pl.ds(half * rows, rows)
        value = (jax.nn.silu(gacc[b % 2, rs]) * uacc[b % 2, rs]).astype(BF16)
        if half == 0:
            hid[:, pl.ds(b * TILE, TILE)] = value
        else:
            hout[b] = value

    for b in range(EARLY):
        for h in range(PARTS):
            if b == 0:
                x_copy(h).wait()
                x_remote(h).start()
            arrive(b, h)
            ask(b * PARTS + h + 1 + AHEAD)
            multiply(b, h, 1, 0, rows)
    half = PARTS // 2
    for b in range(EARLY):
        for at in (0, half):
            if b == 0:
                for h in range(at, at + half):
                    x_remote(h).wait_recv()
                ask(EARLY * PARTS + AHEAD + at + half)
            multiply(b, at, half, rows, rows)
        if b > 0:
            hidden(b - 1, 1)
            hidden(b - 1, 0)
        freed[0] += PARTS
        ask((EARLY + 1) * PARTS + AHEAD)
        if b > 0:
            h_copy(b - 1).start()
    for b in range(EARLY, blocks - 1):
        for h in range(PARTS):
            arrive(b, h)
        ask((b + 1) * PARTS + AHEAD)
        multiply(b, 0, PARTS, 0, 2 * rows)
        hidden(b - 1, 1)
        hidden(b - 1, 0)
        freed[0] += PARTS
        ask((b + 2) * PARTS + AHEAD)
        h_copy(b - 1).start()
    b = blocks - 1
    for at in (0, half):
        for h in range(at, at + half):
            arrive(b, h)
        ask(len(loads))
        multiply(b, at, half, rows, rows)
        if at == 0:
            hidden(b - 1, 1)
            hidden(b - 1, 0)
            h_copy(b - 1).start()
    hidden(b, 1)
    h_copy(b).start()
    multiply(b, 0, PARTS, 0, rows)
    hidden(b, 0)

    def compute(k):
        slot = k % DOWN_SLOTS
        for i in range(2):
            d_copy(k, i).wait()
        if k == 0:
            for b in range(blocks):
                h_copy(b).wait_recv()
        part[k] = dot(hid[...], dbuf[slot])
        if k + DOWN_SLOTS < n:
            for i in range(2):
                d_copy(k + DOWN_SLOTS, i).start()

    plan = reduce_plan(hops)
    place = [{m: q for q, m in enumerate(p)} for p in plan]

    def rs_copy(way, q):
        return pltpu.make_async_remote_copy(
            src_ref=rs_out.at[way, q], dst_ref=rs_in.at[way, q],
            send_sem=rs_send.at[way, q], recv_sem=rs_recv.at[way, q],
            device_id=ways[way], device_id_type=MESH,
        )

    def place_of(way, hop):
        return 0 if hop == 1 else 2 * (hop - 1) - 1 + way

    def reduce_send(way, hop, r):
        q = place[way][hop, r]
        term = part[place_of(way, hop), pl.ds(r * height, height)]
        before = place[way].get((hop - 1, r))
        if before is not None:
            rs_copy(way, before).wait_recv()
            term = term + rs_in[way, before].astype(F32)
        rs_out[way, q] = term.astype(BF16)
        rs_copy(way, q).start()

    def reduce_hop(hop, picked):
        for i in picked:
            for way in range(2):
                order = [r for (h, r) in plan[way] if h == hop]
                reduce_send(way, hop, order[i])

    compute(0)
    reduce_hop(1, range(PIECES // 2))
    compute(1)
    for r in SECOND[0][: PIECES // 2]:
        reduce_send(0, 2, r)
    compute(2)
    for r in SECOND[1][: PIECES // 2]:
        reduce_send(1, 2, r)
    compute(3)
    reduce_hop(2, range(PIECES // 2, PIECES))
    compute(4)
    compute(5)
    reduce_hop(3, range(PIECES // 2))
    compute(6)
    reduce_hop(3, range(PIECES // 2, PIECES))
    compute(7)
    reduce_hop(4, range(PIECES))

    gplan = gather_plan(hops)
    gplace = [{m: q for q, m in enumerate(p)} for p in gplan]

    def ag_copy(way, hop, r):
        q = gplace[way][hop, r]
        back = hop - 1
        owner = lax.rem(tp + (n - back if way == 0 else back), n)
        where = y_ref.at[pl.ds(r * height, height), columns(owner)]
        return pltpu.make_async_remote_copy(
            src_ref=where, dst_ref=where, send_sem=ag_send.at[way, q], recv_sem=ag_recv.at[way, q],
            device_id=ways[way], device_id_type=MESH,
        )

    def ag_arrival(way, hop, r):
        q = gplace[way][hop, r]
        owner = lax.rem(tp + (n - hop if way == 0 else hop), n)
        where = y_ref.at[pl.ds(r * height, height), columns(owner)]
        return pltpu.make_async_remote_copy(
            src_ref=where, dst_ref=where, send_sem=ag_send.at[way, q], recv_sem=ag_recv.at[way, q],
            device_id=ways[way], device_id_type=MESH,
        )

    own = columns(tp)
    for r in FINAL:
        rs = pl.ds(r * height, height)
        total = part[n - 1, rs]
        for way in range(2):
            q = place[way][hops, r]
            rs_copy(way, q).wait_recv()
            total = total + rs_in[way, q].astype(F32)
        y_ref[rs, own] = total.astype(BF16)
        for way in range(2):
            ag_copy(way, 1, r).start()
    for hop in range(1, hops + 1):
        for r in FINAL:
            for way in range(2):
                if (hop, r) in gplace[way]:
                    ag_arrival(way, hop, r).wait_recv()
                    if (hop + 1, r) in gplace[way]:
                        ag_copy(way, hop + 1, r).start()

    for h in range(PARTS):
        x_remote(h).wait_send()
    for b in range(blocks):
        h_copy(b).wait_send()
    for way in range(2):
        for q in range(len(plan[way])):
            rs_copy(way, q).wait_send()
        for hop, r in gplan[way]:
            ag_copy(way, hop, r).wait_send()


def solution(mesh):
    n = mesh.shape["tp"]

    def step(x, w_gate, w_up, w_down):
        rows, depth = x.shape
        cols = w_gate.shape[1]
        mine = cols // 2
        blocks = mine // TILE
        kd = depth // PARTS
        chunk = depth // n
        height = rows // PIECES
        messages = len(reduce_plan(n // 2)[0])
        hbm = pl.BlockSpec(memory_space=pltpu.HBM)
        dma = pltpu.SemaphoreType.DMA
        return pl.pallas_call(
            functools.partial(kernel, n),
            out_shape=pltpu.VMEM((rows, depth), BF16),
            in_specs=[hbm] * 4,
            out_specs=pl.BlockSpec(memory_space=pltpu.VMEM),
            scratch_shapes=[
                pltpu.VMEM((2 * rows, depth), BF16),
                pltpu.VMEM((SLOTS, kd, TILE), BF16),
                pltpu.VMEM((SLOTS, kd, TILE), BF16),
                pltpu.VMEM((2, 2 * rows, TILE), F32),
                pltpu.VMEM((2, 2 * rows, TILE), F32),
                pltpu.VMEM((rows, cols), BF16),
                pltpu.VMEM((blocks, rows, TILE), BF16),
                pltpu.VMEM((DOWN_SLOTS, cols, chunk), BF16),
                pltpu.VMEM((n, rows, chunk), F32),
                pltpu.VMEM((2, messages, height, chunk), BF16),
                pltpu.VMEM((2, messages, height, chunk), BF16),
                dma((PARTS,)), dma((PARTS,)), dma((PARTS,)),
                dma((2, SLOTS)), dma((blocks,)), dma((blocks,)),
                dma((DOWN_SLOTS, 2)),
                dma((2, messages)), dma((2, messages)), dma((2, messages)), dma((2, messages)),
            ],
            compiler_params=pltpu.CompilerParams(
                collective_id=0, has_side_effects=True, vmem_limit_bytes=56 * 1024 * 1024,
            ),
        )(x, w_gate, w_up, w_down)

    return jax.shard_map(
        step,
        mesh=mesh,
        in_specs=(P("dp", None), P(None, "tp"), P(None, "tp"), P("tp", None)),
        out_specs=P("dp", None),
        check_vma=False,
    )
```

```python
import functools

import jax
import jax.numpy as jnp
from jax import lax
from jax.experimental import pallas as pl
from jax.experimental.pallas import tpu as pltpu
from jax.sharding import PartitionSpec as P

MESH = pl.DeviceIdType.MESH
F32, BF16 = jnp.float32, jnp.bfloat16

TILE = 256
PARTS = 4
SLOTS = 12
START = 3
AHEAD = 7
EARLY = 1
DOWN_SLOTS = 4
PIECES = 4

LOWER, UPPER = tuple(range(PIECES // 2)), tuple(range(PIECES // 2, PIECES))


def mixed(a, b):
    return tuple(r for pair in zip(a, b) for r in pair)


FIRST = (LOWER, UPPER)
SECOND = (UPPER + LOWER, LOWER + UPPER)
LATER = (mixed(UPPER, LOWER), mixed(LOWER, UPPER))
FINAL = mixed(LOWER, UPPER)
LAST = (LOWER, UPPER)


def reduce_plan(hops):
    plans = []
    for way in range(2):
        plan = [(1, r) for r in FIRST[way]] + [(2, r) for r in SECOND[way]]
        for hop in range(3, hops + 1):
            plan += [(hop, r) for r in LATER[way]]
        plans.append(plan)
    return plans


def gather_plan(hops):
    plans = []
    for way in range(2):
        plan = [(hop, r) for hop in range(1, hops) for r in FINAL]
        plans.append(plan + [(hops, r) for r in LAST[way]])
    return plans


def kernel(
    n, x_ref, wg_ref, wu_ref, wd_ref, y_ref,
    xs, gbuf, ubuf, gacc, uacc, hid, hout, dbuf, part, rs_out, rs_in,
    x_sem, xr_send, xr_recv, w_sem, h_send, h_recv, d_sem,
    rs_send, rs_recv, ag_send, ag_recv,
):
    rows, depth = x_ref.shape
    cols = wg_ref.shape[1]
    mine = cols // 2
    blocks = mine // TILE
    kd = depth // PARTS
    tiles = kd // TILE
    steps = blocks * PARTS
    chunk = depth // n
    hops = n // 2
    height = rows // PIECES

    tp = lax.axis_index("tp")
    dp = lax.axis_index("dp")
    core = lax.rem(dp, 2)
    partner = {"dp": dp + 1 - 2 * core}
    ways = ({"tp": lax.rem(tp + 1, n)}, {"tp": lax.rem(tp + n - 1, n)})
    my_cols = core * mine
    other_cols = mine - my_cols

    def x_copy(h):
        ks = pl.ds(h * kd, kd)
        return pltpu.make_async_copy(x_ref.at[:, ks], xs.at[pl.ds(0, rows), ks], x_sem.at[h])

    def x_remote(h):
        ks = pl.ds(h * kd, kd)
        return pltpu.make_async_remote_copy(
            src_ref=xs.at[pl.ds(0, rows), ks], dst_ref=xs.at[pl.ds(rows, rows), ks],
            send_sem=xr_send.at[h], recv_sem=xr_recv.at[h], device_id=partner, device_id_type=MESH,
        )

    def w_copies(step):
        b, h, slot = step // PARTS, step % PARTS, step % SLOTS
        ks = pl.ds(h * kd, kd)
        ns = pl.ds(pl.multiple_of(my_cols + b * TILE, TILE), TILE)
        return (
            pltpu.make_async_copy(wg_ref.at[ks, ns], gbuf.at[slot], w_sem.at[0, slot]),
            pltpu.make_async_copy(wu_ref.at[ks, ns], ubuf.at[slot], w_sem.at[1, slot]),
        )

    def chunk_at(k):
        offset = hops if k == 0 else (n if k == n - 1 else (hops - (k + 1) // 2 if k % 2 else n - hops + k // 2))
        return lax.rem(tp + offset, n)

    def columns(c):
        return pl.ds(pl.multiple_of(c * chunk, chunk), chunk)

    def d_copy(k, i):
        slot = k % DOWN_SLOTS
        o = (my_cols, other_cols)[i]
        return pltpu.make_async_copy(
            wd_ref.at[pl.ds(pl.multiple_of(o, mine), mine), columns(chunk_at(k))],
            dbuf.at[slot, pl.ds(i * mine, mine)], d_sem.at[slot, i],
        )

    def h_copy(b):
        return pltpu.make_async_remote_copy(
            src_ref=hout.at[b], dst_ref=hid.at[:, pl.ds(mine + b * TILE, TILE)],
            send_sem=h_send.at[b], recv_sem=h_recv.at[b], device_id=partner, device_id_type=MESH,
        )

    loads = [w_copies(s) for s in range(steps)] + [
        (d_copy(k, i),) for k in range(DOWN_SLOTS) for i in range(2)
    ]
    asked, freed = [0], [0]

    def ask(upto):
        while asked[0] < min(upto, len(loads)) and (asked[0] >= steps or asked[0] < freed[0] + SLOTS):
            for c in loads[asked[0]]:
                c.start()
            asked[0] += 1

    for h in range(PARTS):
        x_copy(h).start()
        ask(min(h + 1, START))

    barrier = pltpu.get_barrier_semaphore()
    for who in (partner,) + ways:
        pl.semaphore_signal(barrier, inc=1, device_id=who, device_id_type=MESH)

    pl.semaphore_wait(barrier, 3)

    def dot(a, b):
        return jnp.dot(a, b, preferred_element_type=F32)

    def arrive(b, h):
        for c in w_copies(b * PARTS + h):
            c.wait()

    def multiply(b, first, count, at, size):
        rs = pl.ds(at, size)
        lhs = xs[rs, pl.ds(first * kd, count * kd)]
        slot = (b * PARTS + first) % SLOTS
        for buf, acc in ((gbuf, gacc), (ubuf, uacc)):
            product = dot(lhs, buf[pl.ds(slot, count)].reshape(count * kd, TILE))
            acc[b % 2, rs] = product if first == 0 else acc[b % 2, rs] + product

    def hidden(b, half):
        rs = pl.ds(half * rows, rows)
        value = (jax.nn.silu(gacc[b % 2, rs]) * uacc[b % 2, rs]).astype(BF16)
        if half == 0:
            hid[:, pl.ds(b * TILE, TILE)] = value
        else:
            hout[b] = value

    for b in range(EARLY):
        for h in range(PARTS):
            if b == 0:
                x_copy(h).wait()
                x_remote(h).start()
            arrive(b, h)
            ask(b * PARTS + h + 1 + AHEAD)
            multiply(b, h, 1, 0, rows)
    half = PARTS // 2
    for b in range(EARLY):
        for at in (0, half):
            if b == 0:
                for h in range(at, at + half):
                    x_remote(h).wait_recv()
                ask(EARLY * PARTS + AHEAD + at + half)
            multiply(b, at, half, rows, rows)
        if b > 0:
            hidden(b - 1, 1)
            hidden(b - 1, 0)
        freed[0] += PARTS
        ask((EARLY + 1) * PARTS + AHEAD)
        if b > 0:
            h_copy(b - 1).start()
    for b in range(EARLY, blocks - 1):
        for at in (0, half):
            for h in range(at, at + half):
                arrive(b, h)
            ask(b * PARTS + at + half + AHEAD)
            multiply(b, at, half, 0, 2 * rows)
            if at == 0:
                hidden(b - 1, 1)
                hidden(b - 1, 0)
            freed[0] += half
            ask(b * PARTS + at + half + AHEAD)
            if at == 0:
                h_copy(b - 1).start()

    b = blocks - 1
    for at in (0, half):
        for h in range(at, at + half):
            arrive(b, h)
        ask(len(loads))
        multiply(b, at, half, rows, rows)
        if at == 0:
            hidden(b - 1, 1)
            hidden(b - 1, 0)
            h_copy(b - 1).start()
    hidden(b, 1)
    h_copy(b).start()
    multiply(b, 0, PARTS, 0, rows)
    hidden(b, 0)

    def compute(k):
        slot = k % DOWN_SLOTS
        for i in range(2):
            d_copy(k, i).wait()
        if k == 0:
            for b in range(blocks):
                h_copy(b).wait_recv()
        part[k] = dot(hid[...], dbuf[slot])
        if k + DOWN_SLOTS < n:
            for i in range(2):
                d_copy(k + DOWN_SLOTS, i).start()

    plan = reduce_plan(hops)
    place = [{m: q for q, m in enumerate(p)} for p in plan]

    def rs_copy(way, q):
        return pltpu.make_async_remote_copy(
            src_ref=rs_out.at[way, q], dst_ref=rs_in.at[way, q],
            send_sem=rs_send.at[way, q], recv_sem=rs_recv.at[way, q],
            device_id=ways[way], device_id_type=MESH,
        )

    def place_of(way, hop):
        return 0 if hop == 1 else 2 * (hop - 1) - 1 + way

    def reduce_send(way, hop, r):
        q = place[way][hop, r]
        term = part[place_of(way, hop), pl.ds(r * height, height)]
        before = place[way].get((hop - 1, r))
        if before is not None:
            rs_copy(way, before).wait_recv()
            term = term + rs_in[way, before].astype(F32)
        rs_out[way, q] = term.astype(BF16)
        rs_copy(way, q).start()

    def reduce_hop(hop, picked):
        for i in picked:
            for way in range(2):
                order = [r for (h, r) in plan[way] if h == hop]
                reduce_send(way, hop, order[i])

    compute(0)
    reduce_hop(1, range(PIECES // 2))
    compute(1)
    for r in SECOND[0][: PIECES // 2]:
        reduce_send(0, 2, r)
    compute(2)
    for r in SECOND[1][: PIECES // 2]:
        reduce_send(1, 2, r)
    compute(3)
    reduce_hop(2, range(PIECES // 2, PIECES))
    compute(4)
    compute(5)
    reduce_hop(3, range(PIECES // 2))
    compute(6)
    reduce_hop(3, range(PIECES // 2, PIECES))
    compute(7)
    reduce_hop(4, range(PIECES))

    gplan = gather_plan(hops)
    gplace = [{m: q for q, m in enumerate(p)} for p in gplan]

    def ag_copy(way, hop, r):
        q = gplace[way][hop, r]
        back = hop - 1
        owner = lax.rem(tp + (n - back if way == 0 else back), n)
        where = y_ref.at[pl.ds(r * height, height), columns(owner)]
        return pltpu.make_async_remote_copy(
            src_ref=where, dst_ref=where, send_sem=ag_send.at[way, q], recv_sem=ag_recv.at[way, q],
            device_id=ways[way], device_id_type=MESH,
        )

    def ag_arrival(way, hop, r):
        q = gplace[way][hop, r]
        owner = lax.rem(tp + (n - hop if way == 0 else hop), n)
        where = y_ref.at[pl.ds(r * height, height), columns(owner)]
        return pltpu.make_async_remote_copy(
            src_ref=where, dst_ref=where, send_sem=ag_send.at[way, q], recv_sem=ag_recv.at[way, q],
            device_id=ways[way], device_id_type=MESH,
        )

    own = columns(tp)
    for r in FINAL:
        rs = pl.ds(r * height, height)
        total = part[n - 1, rs]
        for way in range(2):
            q = place[way][hops, r]
            rs_copy(way, q).wait_recv()
            total = total + rs_in[way, q].astype(F32)
        y_ref[rs, own] = total.astype(BF16)
        for way in range(2):
            ag_copy(way, 1, r).start()
    for hop in range(1, hops + 1):
        for r in FINAL:
            for way in range(2):
                if (hop, r) in gplace[way]:
                    ag_arrival(way, hop, r).wait_recv()
                    if (hop + 1, r) in gplace[way]:
                        ag_copy(way, hop + 1, r).start()

    for h in range(PARTS):
        x_remote(h).wait_send()
    for b in range(blocks):
        h_copy(b).wait_send()
    for way in range(2):
        for q in range(len(plan[way])):
            rs_copy(way, q).wait_send()
        for hop, r in gplan[way]:
            ag_copy(way, hop, r).wait_send()


def solution(mesh):
    n = mesh.shape["tp"]

    def step(x, w_gate, w_up, w_down):
        rows, depth = x.shape
        cols = w_gate.shape[1]
        mine = cols // 2
        blocks = mine // TILE
        kd = depth // PARTS
        chunk = depth // n
        height = rows // PIECES
        messages = len(reduce_plan(n // 2)[0])
        hbm = pl.BlockSpec(memory_space=pltpu.HBM)
        dma = pltpu.SemaphoreType.DMA
        return pl.pallas_call(
            functools.partial(kernel, n),
            out_shape=pltpu.VMEM((rows, depth), BF16),
            in_specs=[hbm] * 4,
            out_specs=pl.BlockSpec(memory_space=pltpu.VMEM),
            scratch_shapes=[
                pltpu.VMEM((2 * rows, depth), BF16),
                pltpu.VMEM((SLOTS, kd, TILE), BF16),
                pltpu.VMEM((SLOTS, kd, TILE), BF16),
                pltpu.VMEM((2, 2 * rows, TILE), F32),
                pltpu.VMEM((2, 2 * rows, TILE), F32),
                pltpu.VMEM((rows, cols), BF16),
                pltpu.VMEM((blocks, rows, TILE), BF16),
                pltpu.VMEM((DOWN_SLOTS, cols, chunk), BF16),
                pltpu.VMEM((n, rows, chunk), F32),
                pltpu.VMEM((2, messages, height, chunk), BF16),
                pltpu.VMEM((2, messages, height, chunk), BF16),
                dma((PARTS,)), dma((PARTS,)), dma((PARTS,)),
                dma((2, SLOTS)), dma((blocks,)), dma((blocks,)),
                dma((DOWN_SLOTS, 2)),
                dma((2, messages)), dma((2, messages)), dma((2, messages)), dma((2, messages)),
            ],
            compiler_params=pltpu.CompilerParams(
                collective_id=0, has_side_effects=True, vmem_limit_bytes=56 * 1024 * 1024,
            ),
        )(x, w_gate, w_up, w_down)

    return jax.shard_map(
        step,
        mesh=mesh,
        in_specs=(P("dp", None), P(None, "tp"), P(None, "tp"), P("tp", None)),
        out_specs=P("dp", None),
        check_vma=False,
    )
```

```python
import functools

import jax
import jax.numpy as jnp
from jax import lax
from jax.experimental import pallas as pl
from jax.experimental.pallas import tpu as pltpu
from jax.sharding import PartitionSpec as P

MESH = pl.DeviceIdType.MESH
F32, BF16 = jnp.float32, jnp.bfloat16

TILE = 256
PARTS = 4
SLOTS = 12
START = 3
AHEAD = 7
EARLY = 1
DOWN_SLOTS = 4
PIECES = 4

LOWER, UPPER = tuple(range(PIECES // 2)), tuple(range(PIECES // 2, PIECES))


def mixed(a, b):
    return tuple(r for pair in zip(a, b) for r in pair)


FIRST = (LOWER, UPPER)
SECOND = (UPPER + LOWER, LOWER + UPPER)
LATER = (mixed(UPPER, LOWER), mixed(LOWER, UPPER))
FINAL = mixed(LOWER, UPPER)
LAST = (LOWER, UPPER)


def reduce_plan(hops):
    plans = []
    for way in range(2):
        plan = [(1, r) for r in FIRST[way]] + [(2, r) for r in SECOND[way]]
        for hop in range(3, hops + 1):
            plan += [(hop, r) for r in LATER[way]]
        plans.append(plan)
    return plans


def gather_plan(hops):
    plans = []
    for way in range(2):
        plan = [(hop, r) for hop in range(1, hops) for r in FINAL]
        plans.append(plan + [(hops, r) for r in LAST[way]])
    return plans


def kernel(
    n, x_ref, wg_ref, wu_ref, wd_ref, y_ref,
    xs, gbuf, ubuf, gacc, uacc, hid, hout, dbuf, part, rs_out, rs_in,
    x_sem, xr_send, xr_recv, w_sem, h_send, h_recv, d_sem,
    rs_send, rs_recv, ag_send, ag_recv,
):
    rows, depth = x_ref.shape
    cols = wg_ref.shape[1]
    mine = cols // 2
    blocks = mine // TILE
    kd = depth // PARTS
    tiles = kd // TILE
    steps = blocks * PARTS
    chunk = depth // n
    hops = n // 2
    height = rows // PIECES

    tp = lax.axis_index("tp")
    dp = lax.axis_index("dp")
    core = lax.rem(dp, 2)
    partner = {"dp": dp + 1 - 2 * core}
    ways = ({"tp": lax.rem(tp + 1, n)}, {"tp": lax.rem(tp + n - 1, n)})
    my_cols = core * mine
    other_cols = mine - my_cols

    def x_copy(h):
        ks = pl.ds(h * kd, kd)
        return pltpu.make_async_copy(x_ref.at[:, ks], xs.at[pl.ds(0, rows), ks], x_sem.at[h])

    def x_remote(h):
        ks = pl.ds(h * kd, kd)
        return pltpu.make_async_remote_copy(
            src_ref=xs.at[pl.ds(0, rows), ks], dst_ref=xs.at[pl.ds(rows, rows), ks],
            send_sem=xr_send.at[h], recv_sem=xr_recv.at[h], device_id=partner, device_id_type=MESH,
        )

    def w_copies(step):
        b, h, slot = step // PARTS, step % PARTS, step % SLOTS
        ks = pl.ds(h * kd, kd)
        ns = pl.ds(pl.multiple_of(my_cols + b * TILE, TILE), TILE)
        return (
            pltpu.make_async_copy(wg_ref.at[ks, ns], gbuf.at[slot], w_sem.at[0, slot]),
            pltpu.make_async_copy(wu_ref.at[ks, ns], ubuf.at[slot], w_sem.at[1, slot]),
        )

    def chunk_at(k):
        offset = hops if k == 0 else (n if k == n - 1 else (hops - (k + 1) // 2 if k % 2 else n - hops + k // 2))
        return lax.rem(tp + offset, n)

    def columns(c):
        return pl.ds(pl.multiple_of(c * chunk, chunk), chunk)

    def d_copy(k, i):
        slot = k % DOWN_SLOTS
        o = (my_cols, other_cols)[i]
        return pltpu.make_async_copy(
            wd_ref.at[pl.ds(pl.multiple_of(o, mine), mine), columns(chunk_at(k))],
            dbuf.at[slot, pl.ds(i * mine, mine)], d_sem.at[slot, i],
        )

    def h_copy(b):
        return pltpu.make_async_remote_copy(
            src_ref=hout.at[b], dst_ref=hid.at[:, pl.ds(mine + b * TILE, TILE)],
            send_sem=h_send.at[b], recv_sem=h_recv.at[b], device_id=partner, device_id_type=MESH,
        )

    loads = [w_copies(s) for s in range(steps)] + [
        (d_copy(k, i),) for k in range(DOWN_SLOTS) for i in range(2)
    ]
    asked, freed = [0], [0]

    def ask(upto):
        while asked[0] < min(upto, len(loads)) and (asked[0] >= steps or asked[0] < freed[0] + SLOTS):
            for c in loads[asked[0]]:
                c.start()
            asked[0] += 1

    for h in range(PARTS):
        x_copy(h).start()
        ask(min(h + 1, START))

    barrier = pltpu.get_barrier_semaphore()
    for who in (partner,) + ways:
        pl.semaphore_signal(barrier, inc=1, device_id=who, device_id_type=MESH)

    pl.semaphore_wait(barrier, 3)

    def dot(a, b):
        return jnp.dot(a, b, preferred_element_type=F32)

    def arrive(b, h):
        for c in w_copies(b * PARTS + h):
            c.wait()

    def multiply(b, first, count, at, size):
        rs = pl.ds(at, size)
        lhs = xs[rs, pl.ds(first * kd, count * kd)]
        slot = (b * PARTS + first) % SLOTS
        for buf, acc in ((gbuf, gacc), (ubuf, uacc)):
            product = dot(lhs, buf[pl.ds(slot, count)].reshape(count * kd, TILE))
            acc[b % 2, rs] = product if first == 0 else acc[b % 2, rs] + product

    def hidden(b, half):
        rs = pl.ds(half * rows, rows)
        value = (jax.nn.silu(gacc[b % 2, rs]) * uacc[b % 2, rs]).astype(BF16)
        if half == 0:
            hid[:, pl.ds(b * TILE, TILE)] = value
        else:
            hout[b] = value

    for b in range(EARLY):
        for h in range(PARTS):
            if b == 0:
                x_copy(h).wait()
                x_remote(h).start()
            arrive(b, h)
            ask(b * PARTS + h + 1 + AHEAD)
            multiply(b, h, 1, 0, rows)
    half = PARTS // 2
    for b in range(EARLY):
        for at in (0, half):
            if b == 0:
                for h in range(at, at + half):
                    x_remote(h).wait_recv()
                ask(EARLY * PARTS + AHEAD + at + half)
            multiply(b, at, half, rows, rows)
        if b > 0:
            hidden(b - 1, 1)
            hidden(b - 1, 0)
        freed[0] += PARTS
        ask((EARLY + 1) * PARTS + AHEAD)
        if b > 0:
            h_copy(b - 1).start()
    for b in range(EARLY, blocks - 1):
        for at in (0, half):
            for h in range(at, at + half):
                arrive(b, h)
            ask(b * PARTS + at + half + AHEAD)
            multiply(b, at, half, 0, 2 * rows)
            if at == 0:
                hidden(b - 1, 1)
                hidden(b - 1, 0)
            freed[0] += half
            ask(b * PARTS + at + half + AHEAD)
            if at == 0:
                h_copy(b - 1).start()

    b = blocks - 1
    for at in (0, half):
        for h in range(at, at + half):
            arrive(b, h)
        ask(len(loads))
        multiply(b, at, half, rows, rows)
        if at == 0:
            hidden(b - 1, 1)
            hidden(b - 1, 0)
            h_copy(b - 1).start()
    hidden(b, 1)
    h_copy(b).start()
    multiply(b, 0, PARTS, 0, rows)
    hidden(b, 0)

    def compute(k):
        slot = k % DOWN_SLOTS
        for i in range(2):
            d_copy(k, i).wait()
        if k == 0:
            for b in range(blocks):
                h_copy(b).wait_recv()
        part[k] = dot(hid[...], dbuf[slot])
        if k + DOWN_SLOTS < n:
            for i in range(2):
                d_copy(k + DOWN_SLOTS, i).start()

    plan = reduce_plan(hops)
    place = [{m: q for q, m in enumerate(p)} for p in plan]

    def rs_copy(way, q):
        return pltpu.make_async_remote_copy(
            src_ref=rs_out.at[way, q], dst_ref=rs_in.at[way, q],
            send_sem=rs_send.at[way, q], recv_sem=rs_recv.at[way, q],
            device_id=ways[way], device_id_type=MESH,
        )

    def place_of(way, hop):
        return 0 if hop == 1 else 2 * (hop - 1) - 1 + way

    def reduce_send(way, hop, r):
        q = place[way][hop, r]
        term = part[place_of(way, hop), pl.ds(r * height, height)]
        before = place[way].get((hop - 1, r))
        if before is not None:
            rs_copy(way, before).wait_recv()
            term = term + rs_in[way, before].astype(F32)
        rs_out[way, q] = term.astype(BF16)
        rs_copy(way, q).start()

    def reduce_hop(hop, picked):
        for i in picked:
            for way in range(2):
                order = [r for (h, r) in plan[way] if h == hop]
                reduce_send(way, hop, order[i])

    compute(0)
    reduce_hop(1, range(PIECES // 2))
    compute(1)
    for r in SECOND[0][: PIECES // 2]:
        reduce_send(0, 2, r)
    compute(2)
    for r in SECOND[1][: PIECES // 2]:
        reduce_send(1, 2, r)
    compute(3)
    reduce_hop(2, range(PIECES // 2, PIECES))
    compute(4)
    compute(5)
    reduce_hop(3, range(PIECES // 2))
    compute(6)
    reduce_hop(3, range(PIECES // 2, PIECES))
    compute(7)
    reduce_hop(4, range(PIECES))

    gplan = gather_plan(hops)
    gplace = [{m: q for q, m in enumerate(p)} for p in gplan]

    def ag_copy(way, hop, r):
        q = gplace[way][hop, r]
        back = hop - 1
        owner = lax.rem(tp + (n - back if way == 0 else back), n)
        where = y_ref.at[pl.ds(r * height, height), columns(owner)]
        return pltpu.make_async_remote_copy(
            src_ref=where, dst_ref=where, send_sem=ag_send.at[way, q], recv_sem=ag_recv.at[way, q],
            device_id=ways[way], device_id_type=MESH,
        )

    def ag_arrival(way, hop, r):
        q = gplace[way][hop, r]
        owner = lax.rem(tp + (n - hop if way == 0 else hop), n)
        where = y_ref.at[pl.ds(r * height, height), columns(owner)]
        return pltpu.make_async_remote_copy(
            src_ref=where, dst_ref=where, send_sem=ag_send.at[way, q], recv_sem=ag_recv.at[way, q],
            device_id=ways[way], device_id_type=MESH,
        )

    own = columns(tp)
    for r in FINAL:
        rs = pl.ds(r * height, height)
        total = part[n - 1, rs]
        for way in range(2):
            q = place[way][hops, r]
            rs_copy(way, q).wait_recv()
            total = total + rs_in[way, q].astype(F32)
        y_ref[rs, own] = total.astype(BF16)
        for way in range(2):
            ag_copy(way, 1, r).start()
    for h in range(PARTS):
        x_remote(h).wait_send()
    for b in range(blocks):
        h_copy(b).wait_send()
    for way in range(2):
        for q in range(len(plan[way])):
            rs_copy(way, q).wait_send()
    for hop in range(1, hops + 1):
        for r in FINAL:
            for way in range(2):
                if (hop, r) in gplace[way]:
                    ag_arrival(way, hop, r).wait_recv()
                    if (hop + 1, r) in gplace[way]:
                        ag_copy(way, hop + 1, r).start()

    for way in range(2):
        for hop, r in gplan[way]:
            ag_copy(way, hop, r).wait_send()


def solution(mesh):
    n = mesh.shape["tp"]

    def step(x, w_gate, w_up, w_down):
        rows, depth = x.shape
        cols = w_gate.shape[1]
        mine = cols // 2
        blocks = mine // TILE
        kd = depth // PARTS
        chunk = depth // n
        height = rows // PIECES
        messages = len(reduce_plan(n // 2)[0])
        hbm = pl.BlockSpec(memory_space=pltpu.HBM)
        dma = pltpu.SemaphoreType.DMA
        return pl.pallas_call(
            functools.partial(kernel, n),
            out_shape=pltpu.VMEM((rows, depth), BF16),
            in_specs=[hbm] * 4,
            out_specs=pl.BlockSpec(memory_space=pltpu.VMEM),
            scratch_shapes=[
                pltpu.VMEM((2 * rows, depth), BF16),
                pltpu.VMEM((SLOTS, kd, TILE), BF16),
                pltpu.VMEM((SLOTS, kd, TILE), BF16),
                pltpu.VMEM((2, 2 * rows, TILE), F32),
                pltpu.VMEM((2, 2 * rows, TILE), F32),
                pltpu.VMEM((rows, cols), BF16),
                pltpu.VMEM((blocks, rows, TILE), BF16),
                pltpu.VMEM((DOWN_SLOTS, cols, chunk), BF16),
                pltpu.VMEM((n, rows, chunk), F32),
                pltpu.VMEM((2, messages, height, chunk), BF16),
                pltpu.VMEM((2, messages, height, chunk), BF16),
                dma((PARTS,)), dma((PARTS,)), dma((PARTS,)),
                dma((2, SLOTS)), dma((blocks,)), dma((blocks,)),
                dma((DOWN_SLOTS, 2)),
                dma((2, messages)), dma((2, messages)), dma((2, messages)), dma((2, messages)),
            ],
            compiler_params=pltpu.CompilerParams(
                collective_id=0, has_side_effects=True, vmem_limit_bytes=56 * 1024 * 1024,
            ),
        )(x, w_gate, w_up, w_down)

    return jax.shard_map(
        step,
        mesh=mesh,
        in_specs=(P("dp", None), P(None, "tp"), P(None, "tp"), P("tp", None)),
        out_specs=P("dp", None),
        check_vma=False,
    )
```
